32 devices in a mesh: groups: 2 (over y), res: 8 (over z, x), seq: 2 (over core).
Axes of the slice: x: 2, y: 2, z: 4, core: 2. Of those that a mesh axis runs over, the one named last changes fastest.
Arguments:
- alignment: bfloat16 [128, 32, 256], P(('groups', 'seq'), 'res'), parts along dimension 0, may hold values from -6 to 6
- ln_gain: float32 [256], replicated, may hold values from 0.1 to 1.9
- proj_left: bfloat16 [256, 32], replicated, may hold values from -0.375 to 0.375
- proj_right: bfloat16 [256, 32], replicated, may hold values from -0.375 to 0.375
- out_weight: bfloat16 [1024, 128], replicated, may hold values from -4 to 4
- out_bias: float32 [128], replicated, may hold values from -3 to 3
Outputs:
- pair_update: bfloat16 [64, 32, 128], P(('groups', 'res'), 'seq'), parts along dimension 0
The draws below stay inside these ranges and needn't reach their ends.
There are 2 independent parts, one for each index of `groups`. The reference program is written for one: setup_inputs(seed, part) draws one part's arguments, and reference() takes and returns one part's arrays. A program takes and returns all parts, laid end to end along the dimension named above; an argument that names none is the same for every part. Nothing has to cross between parts.
All inputs are finite; a program needn't handle non-finite values.
Results may differ from the reference program's by a relative error of at most 0.0095.
Values may be sent and summed in bfloat16 or wider, within the bound.
A program may use at most 64 MiB of HBM per device.

```python
import math
import jax
import jax.numpy as jnp
from jax import lax

CM = 256
CH = 32
CZ = 128
SEQS = 64
RES = 32


def steps_of(rng, dims, cuts, smallest, largest):
    loudness, own = 1.0, jax.random.fold_in(rng, 6)
    for axis_at, blocks in cuts:
        draws = jnp.exp(jax.random.uniform(jax.random.fold_in(own, axis_at), (blocks,), jnp.float32, smallest / len(cuts), largest / len(cuts)))
        loudness = loudness * jnp.repeat(draws, dims[axis_at] // blocks).reshape([-1 if axis == axis_at else 1 for axis in range(len(dims))])
    return loudness


def normal_values(key, shape, width, most, shards=(), kind=jnp.bfloat16):
    values = width * jax.random.normal(key, shape, jnp.float32)
    if shards:
        values = values * steps_of(key, shape, shards, -0.22, 0.18)
    return jnp.clip(values, -most, most).astype(kind)


def setup_inputs(seed: int = 0, part: int = 0) -> dict:
    splits = jax.random.split(jax.random.key(seed), 7)
    part_keys = jax.random.split(jax.random.fold_in(splits[6], part), 7)
    return {
        "alignment": normal_values(part_keys[0], (SEQS, RES, CM), 1.0, 6.0, ((0, 2), (1, 8))),
        "ln_gain": jnp.clip(1.0 + 0.18 * jax.random.normal(splits[1], (CM,), jnp.float32), 0.1, 1.9),
        "proj_left": normal_values(splits[2], (CM, CH), CM ** -0.5, 0.375),
        "proj_right": normal_values(splits[3], (CM, CH), CM ** -0.5, 0.375),
        "out_weight": normal_values(splits[4], (CH * CH, CZ), (SEQS ** 0.5 / CH), 4.0),
        "out_bias": normal_values(splits[5], (CZ,), 0.5, 3.0, (), jnp.float32),
    }


def normalize(alignment, ln_gain):
    values = alignment.astype(jnp.float32)
    centred = values - lax.optimization_barrier(jnp.mean(values, axis=-1, keepdims=True))
    variance = lax.optimization_barrier(jnp.mean(centred * centred, axis=-1, keepdims=True))
    return (centred * lax.rsqrt(variance + 1e-05) * ln_gain).astype(jnp.bfloat16)

def project_in(normed, weight):
    flat_rows = normed.reshape(-1, normed.shape[2])
    projected = jnp.dot(flat_rows, weight, preferred_element_type=jnp.float32).astype(jnp.bfloat16)
    return projected.reshape(normed.shape[0], normed.shape[1], weight.shape[1])

def reference(alignment, ln_gain, proj_left, proj_right, out_weight, out_bias):
    normed = normalize(alignment, ln_gain)
    left_side = project_in(normed, proj_left)
    right_side = project_in(normed, proj_right)
    right_flat = right_side.reshape(SEQS, RES * CH)
    weight_full = out_weight.astype(jnp.float32)
    block_width = math.gcd(RES, 8)

    def row_block(position):
        picked = lax.dynamic_slice_in_dim(left_side, position * block_width, block_width, 1)
        picked = picked.reshape(SEQS, block_width * CH)
        outer_terms = lax.dot_general(picked, right_flat, (((0,), (0,)), ((), ())), preferred_element_type=jnp.float32) * (1.0 / SEQS)
        outer_terms = outer_terms.reshape(block_width, CH, RES, CH).transpose(0, 2, 1, 3).reshape(block_width * RES, CH * CH)
        projected = jnp.dot(outer_terms, weight_full, precision=lax.Precision.HIGHEST) + out_bias
        return projected.reshape(block_width, RES, CZ).astype(jnp.bfloat16)
    blocks = lax.map(row_block, jnp.arange(RES // block_width, dtype=jnp.int32))
    return blocks.reshape(RES, RES, CZ)
```

```python
import functools
import math

import jax
import jax.numpy as jnp
from jax import lax
from jax.experimental import pallas as pl
from jax.experimental.pallas import tpu as pltpu
from jax.sharding import PartitionSpec as P

F32 = jnp.float32
BF16 = jnp.bfloat16
MESH = pl.DeviceIdType.MESH
LANES = 128
SUBLANES = 8


def dot_last(a, b):
    return lax.dot_general(a, b, (((1,), (1,)), ((), ())), preferred_element_type=F32)


def dot(a, b):
    return jnp.dot(a, b, preferred_element_type=F32)


def kernel(
    n_res, n_seq, x_hbm, gain_hbm, wl_hbm, wr_hbm, w_hbm, bias_hbm, out_ref,
    x_ref, gain_ref, wl_ref, wr_ref, w_ref, bias_ref,
    norm_ref, wide_ref, mixed_ref, left_own, left_got, blocks, right_own, right_got, terms,
    load_sem, lsend_sem, lrecv_sem, rsend_sem, rrecv_sem, self_sem,
):
    seqs, res, width = x_ref.shape
    ch = wl_ref.shape[1]
    cz = w_ref.shape[1]
    pack = LANES // seqs
    high = ch // pack
    half = n_res // n_seq
    rows = res * high
    inv_count = 1.0 / (seqs * n_seq)
    my_res, my_seq = lax.axis_index("res"), lax.axis_index("seq")
    my_col = my_res // half
    first = my_seq * half

    loads = [
        pltpu.make_async_copy(src, dst, load_sem.at[n])
        for n, (src, dst) in enumerate(
            (
                (x_hbm, x_ref),
                (gain_hbm, gain_ref),
                (wr_hbm, wr_ref),
                (wl_hbm, wl_ref),
                (w_hbm, w_ref),
                (bias_hbm, bias_ref),
            )
        )
    ]
    for load in loads:
        load.start()

    barrier = pltpu.get_barrier_semaphore()

    def greet(res_at, seq_at):
        pl.semaphore_signal(
            barrier, inc=1, device_id={"res": res_at, "seq": seq_at}, device_id_type=MESH
        )

    for k in range(1, n_seq):
        greet(my_res, lax.rem(my_seq + k, n_seq))

    def greet_block(n, carry):
        res_at = first + n

        for k in range(n_seq):

            @pl.when(res_at != my_res)
            def _():
                greet(res_at, lax.rem(my_seq + k, n_seq))

        return carry

    lax.fori_loop(0, half, greet_block, 0, unroll=half <= 8)

    loads[2].wait()
    at_row = lax.broadcasted_iota(jnp.int32, (ch, ch), 0)
    at_col = lax.broadcasted_iota(jnp.int32, (ch, ch), 1)
    shuffle = (at_col == (at_row % high) * pack + at_row // high).astype(F32).astype(BF16)
    wr_rows = dot_last(shuffle, wr_ref[...]).astype(BF16)

    loads[0].wait()
    loads[1].wait()
    values = x_ref[...].astype(F32).reshape(seqs * res, width)
    centred = values - jnp.mean(values, axis=-1, keepdims=True)
    variance = jnp.mean(centred * centred, axis=-1, keepdims=True)
    scaled = (centred * lax.rsqrt(variance + 1e-05)) * gain_ref[...]
    for n in range(width // LANES):
        norm_ref[n] = scaled[:, n * LANES : (n + 1) * LANES]
    normed = jnp.concatenate(
        [
            jnp.concatenate(
                [
                    norm_ref[n, pl.ds(i, seqs, stride=res), :].astype(BF16)
                    for n in range(width // LANES)
                ],
                1,
            )
            for i in range(res)
        ],
        0,
    )

    right = dot_last(wr_rows, normed)
    lane_group = lax.broadcasted_iota(jnp.int32, (high, LANES), 1) // seqs
    for j in range(res):
        total = None
        for g in range(pack):
            piece = right[g * high : (g + 1) * high]
            shift = (g - j) * seqs % LANES
            if shift:
                piece = pltpu.roll(piece, shift, 1)
            total = piece if total is None else jnp.where(lane_group == g, piece, total)
        right_own[j * high : (j + 1) * high, :] = total.astype(BF16)

    pl.semaphore_wait(barrier, n_res + n_seq - 2)

    my_slot = lax.rem(my_res, half)
    away = lax.rem(my_seq - my_col + n_seq, n_seq)

    def slot_at(slot, part):
        return right_got.at[slot, :, pl.ds(pl.multiple_of(part * LANES, LANES), LANES)]

    def send_right(step):
        return pltpu.make_async_remote_copy(
            src_ref=right_own,
            dst_ref=slot_at(my_slot, away),
            send_sem=rsend_sem.at[step],
            recv_sem=rrecv_sem.at[my_slot, away],
            device_id={"res": lax.rem(my_res + step, n_res), "seq": my_col},
            device_id_type=MESH,
        )

    def start_right(n, carry):
        send_right(n + 1).start()
        return carry

    lax.fori_loop(0, n_res - 1, start_right, 0, unroll=n_res <= 8)
    keep = pltpu.make_async_copy(right_own, slot_at(my_slot, 0), self_sem)

    @pl.when(away == 0)
    def _():
        keep.start()

    @pl.when(away != 0)
    def _():
        send_right(0).start()

    loads[3].wait()
    spread = (
        lax.broadcasted_iota(jnp.int32, (ch, pack * ch), 1) % ch
        == lax.broadcasted_iota(jnp.int32, (ch, pack * ch), 0)
    ).astype(F32).astype(BF16)
    wl_wide = dot(wl_ref[...], spread).astype(BF16)
    left_own[...] = dot(normed, wl_wide).astype(BF16)
    left_sends = []
    for k in range(1, n_seq):
        copy = pltpu.make_async_remote_copy(
            src_ref=left_own,
            dst_ref=left_got.at[n_seq - k - 1],
            send_sem=lsend_sem.at[k - 1],
            recv_sem=lrecv_sem.at[n_seq - k - 1],
            device_id={"res": my_res, "seq": lax.rem(my_seq + k, n_seq)},
            device_id_type=MESH,
        )
        copy.start()
        left_sends.append(copy)

    loads[4].wait()
    loads[5].wait()
    wide_ref[...] = w_ref[...].astype(F32)
    for e in range(ch):
        mixed_ref[e * ch : (e + 1) * ch, :] = wide_ref[pl.ds(e, ch, stride=ch), :].astype(BF16)

    masks = [
        (lax.broadcasted_iota(jnp.int32, (seqs, pack * ch), 1) // ch == g).astype(F32).astype(BF16)
        for g in range(pack)
    ]

    def place(part, source):
        for i in range(res):
            block = source[i * seqs : (i + 1) * seqs, :]
            for g in range(pack):
                at = part * LANES + g * seqs
                blocks[at : at + seqs, i * pack * ch : (i + 1) * pack * ch] = block * masks[g]

    place(0, left_own)
    for k in range(1, n_seq):
        left_sends[n_seq - k - 1].wait_recv()
        place(k, left_got.at[k - 1])

    group = math.gcd(half, 4)

    def columns(n):
        for m in range(group):
            slot = n * group + m
            for part in range(n_seq):

                def arrived():
                    pltpu.make_async_remote_copy(
                        src_ref=right_own,
                        dst_ref=slot_at(slot, part),
                        send_sem=rsend_sem.at[0],
                        recv_sem=rrecv_sem.at[slot, part],
                        device_id={"res": my_res, "seq": my_col},
                        device_id_type=MESH,
                    ).wait_recv()

                if part:
                    arrived()
                else:
                    mine = first + slot == my_res
                    pl.when(mine)(keep.wait)
                    pl.when(jnp.logical_not(mine))(arrived)
        got = right_got[pl.ds(n * group, group)].reshape(group * rows, n_seq * LANES)
        outer = dot(got, blocks[...]) * inv_count
        for i in range(res):
            terms[i] = outer[:, i * LANES : (i + 1) * LANES]
        count = group * res
        lhs = jnp.concatenate(
            [
                jnp.concatenate(
                    [
                        terms[i, pl.ds(h, count, stride=high), :].astype(BF16)
                        for h in range(high)
                    ],
                    1,
                )
                for i in range(res)
            ],
            0,
        )
        result = dot(lhs, mixed_ref[...]) + bias_ref[...]
        for i in range(res):
            at = pl.ds(pl.multiple_of(n * count, count), count)
            out_ref[i, at, :] = result[i * count : (i + 1) * count].astype(out_ref.dtype)

    if half == group:
        columns(0)
    else:

        @pl.loop(0, half // group)
        def _(n):
            columns(n)

    for copy in left_sends:
        copy.wait_send()

    def finish_right(n, carry):
        send_right(n + 1).wait_send()
        return carry

    lax.fori_loop(0, n_res - 1, finish_right, 0, unroll=n_res <= 8)

    @pl.when(away != 0)
    def _():
        send_right(0).wait_send()


def on_device(alignment, ln_gain, proj_left, proj_right, out_weight, out_bias):
    n_res, n_seq = lax.axis_size("res"), lax.axis_size("seq")
    seqs, res, width = alignment.shape
    ch = proj_left.shape[1]
    cz = out_weight.shape[1]
    half = n_res // n_seq
    cols = res * half
    pack = LANES // seqs
    rows = res * (ch // pack)
    wide = res * pack * ch
    group = math.gcd(half, 4)
    return pl.pallas_call(
        functools.partial(kernel, n_res, n_seq),
        out_shape=jax.ShapeDtypeStruct((res, cols, cz), BF16),
        in_specs=[pl.BlockSpec(memory_space=pl.ANY)] * 6,
        out_specs=pl.BlockSpec(memory_space=pltpu.VMEM),
        scratch_shapes=[
            pltpu.VMEM((seqs, res, width), BF16),
            pltpu.VMEM((1, width), F32),
            pltpu.VMEM((width, ch), BF16),
            pltpu.VMEM((width, ch), BF16),
            pltpu.VMEM((ch * ch, cz), BF16),
            pltpu.VMEM((1, cz), F32),
            pltpu.VMEM((width // LANES, seqs * res, LANES), F32),
            pltpu.VMEM((ch * ch, cz), F32),
            pltpu.VMEM((ch * ch, cz), BF16),
            pltpu.VMEM((res * seqs, pack * ch), BF16),
            pltpu.VMEM((n_seq - 1, res * seqs, pack * ch), BF16),
            pltpu.VMEM((n_seq * LANES, wide), BF16),
            pltpu.VMEM((rows, LANES), BF16),
            pltpu.VMEM((half, rows, n_seq * LANES), BF16),
            pltpu.VMEM((res, group * rows, LANES), F32),
            pltpu.SemaphoreType.DMA((6,)),
            pltpu.SemaphoreType.DMA((n_seq - 1,)),
            pltpu.SemaphoreType.DMA((n_seq - 1,)),
            pltpu.SemaphoreType.DMA((n_res,)),
            pltpu.SemaphoreType.DMA((half, n_seq)),
            pltpu.SemaphoreType.DMA,
        ],
        compiler_params=pltpu.CompilerParams(collective_id=0, has_side_effects=True),
    )(
        alignment,
        ln_gain.reshape(1, width),
        proj_left,
        proj_right,
        out_weight,
        out_bias.reshape(1, cz),
    )


def solution(mesh):
    placed = (P(("groups", "seq"), "res", None), P(), P(), P(), P(), P())
    return jax.shard_map(
        on_device,
        mesh=mesh,
        in_specs=placed,
        out_specs=P(("groups", "res"), "seq", None),
        check_vma=False,
    )
```

```python
import functools
import math

import jax
import jax.numpy as jnp
from jax import lax
from jax.experimental import pallas as pl
from jax.experimental.pallas import tpu as pltpu
from jax.sharding import PartitionSpec as P

F32 = jnp.float32
BF16 = jnp.bfloat16
MESH = pl.DeviceIdType.MESH
LANES = 128
SUBLANES = 8


def dot_last(a, b):
    return lax.dot_general(a, b, (((1,), (1,)), ((), ())), preferred_element_type=F32)


def dot(a, b):
    return jnp.dot(a, b, preferred_element_type=F32)


def kernel(
    n_res, n_seq, x_hbm, gain_hbm, wl_hbm, wr_hbm, w_hbm, bias_hbm, out_ref,
    x_ref, gain_ref, wl_ref, wr_ref, w_ref, bias_ref,
    norm_ref, wide_ref, mixed_ref, left_own, left_got, blocks, right_own, right_got, terms,
    load_sem, lsend_sem, lrecv_sem, rsend_sem, rrecv_sem, self_sem,
):
    seqs, res, width = x_ref.shape
    ch = wl_ref.shape[0]
    pack = LANES // seqs
    high = ch // pack
    half = n_res // n_seq
    rows = res * high
    inv_count = 1.0 / (seqs * n_seq)
    my_res, my_seq = lax.axis_index("res"), lax.axis_index("seq")
    my_col = my_res // half
    first = my_seq * half

    loads = [
        pltpu.make_async_copy(src, dst, load_sem.at[n])
        for n, (src, dst) in enumerate(
            (
                (x_hbm, x_ref),
                (gain_hbm, gain_ref),
                (wr_hbm, wr_ref),
                (wl_hbm, wl_ref),
                (w_hbm, w_ref),
                (bias_hbm, bias_ref),
            )
        )
    ]
    for load in loads:
        load.start()

    barrier = pltpu.get_barrier_semaphore()

    def greet(res_at, seq_at):
        pl.semaphore_signal(
            barrier, inc=1, device_id={"res": res_at, "seq": seq_at}, device_id_type=MESH
        )

    for k in range(1, n_seq):
        greet(my_res, lax.rem(my_seq + k, n_seq))

    def greet_block(n, carry):
        res_at = first + n

        for k in range(n_seq):

            @pl.when(res_at != my_res)
            def _():
                greet(res_at, lax.rem(my_seq + k, n_seq))

        return carry

    lax.fori_loop(0, half, greet_block, 0, unroll=half <= 8)

    loads[2].wait()
    at_row = lax.broadcasted_iota(jnp.int32, (ch, ch), 0)
    at_col = lax.broadcasted_iota(jnp.int32, (ch, ch), 1)
    shuffle = (at_col == (at_row % high) * pack + at_row // high).astype(F32).astype(BF16)
    wr_rows = dot(shuffle, wr_ref[...]).astype(BF16)

    loads[0].wait()
    loads[1].wait()
    values = x_ref[...].astype(F32).reshape(seqs * res, width)
    centred = values - jnp.mean(values, axis=-1, keepdims=True)
    variance = jnp.mean(centred * centred, axis=-1, keepdims=True)
    scaled = (centred * lax.rsqrt(variance + 1e-05)) * gain_ref[...]
    for n in range(width // LANES):
        norm_ref[n] = scaled[:, n * LANES : (n + 1) * LANES]
    normed = jnp.concatenate(
        [
            jnp.concatenate(
                [
                    norm_ref[n, pl.ds(i, seqs, stride=res), :].astype(BF16)
                    for n in range(width // LANES)
                ],
                1,
            )
            for i in range(res)
        ],
        0,
    )

    right = dot_last(wr_rows, normed)
    lane_group = lax.broadcasted_iota(jnp.int32, (high, LANES), 1) // seqs
    for j in range(res):
        total = None
        for g in range(pack):
            piece = right[g * high : (g + 1) * high]
            shift = (g - j) * seqs % LANES
            if shift:
                piece = pltpu.roll(piece, shift, 1)
            total = piece if total is None else jnp.where(lane_group == g, piece, total)
        right_own[j * high : (j + 1) * high, :] = total.astype(BF16)

    pl.semaphore_wait(barrier, n_res + n_seq - 2)

    my_slot = lax.rem(my_res, half)
    away = lax.rem(my_seq - my_col + n_seq, n_seq)

    def slot_at(slot, part):
        return right_got.at[slot, :, pl.ds(pl.multiple_of(part * LANES, LANES), LANES)]

    def send_right(step):
        return pltpu.make_async_remote_copy(
            src_ref=right_own,
            dst_ref=slot_at(my_slot, away),
            send_sem=rsend_sem.at[step],
            recv_sem=rrecv_sem.at[my_slot, away],
            device_id={"res": lax.rem(my_res + step, n_res), "seq": my_col},
            device_id_type=MESH,
        )

    def start_right(n, carry):
        send_right(n + 1).start()
        return carry

    lax.fori_loop(0, n_res - 1, start_right, 0, unroll=n_res <= 8)
    keep = pltpu.make_async_copy(right_own, slot_at(my_slot, 0), self_sem)

    @pl.when(away == 0)
    def _():
        keep.start()

    @pl.when(away != 0)
    def _():
        send_right(0).start()

    loads[3].wait()
    wl_wide = jnp.concatenate([wl_ref[...]] * pack, 0)
    left_own[...] = dot_last(normed, wl_wide).astype(BF16)
    left_sends = []
    for k in range(1, n_seq):
        copy = pltpu.make_async_remote_copy(
            src_ref=left_own,
            dst_ref=left_got.at[n_seq - k - 1],
            send_sem=lsend_sem.at[k - 1],
            recv_sem=lrecv_sem.at[n_seq - k - 1],
            device_id={"res": my_res, "seq": lax.rem(my_seq + k, n_seq)},
            device_id_type=MESH,
        )
        copy.start()
        left_sends.append(copy)

    loads[4].wait()
    loads[5].wait()
    wide_ref[...] = w_ref[...].astype(F32)
    for e in range(ch):
        mixed_ref[e * ch : (e + 1) * ch, :] = wide_ref[pl.ds(e, ch, stride=ch), :].astype(BF16)

    masks = [
        (lax.broadcasted_iota(jnp.int32, (seqs, pack * ch), 1) // ch == g).astype(F32).astype(BF16)
        for g in range(pack)
    ]

    def place(part, source):
        for i in range(res):
            block = source[i * seqs : (i + 1) * seqs, :]
            for g in range(pack):
                at = part * LANES + g * seqs
                blocks[at : at + seqs, i * pack * ch : (i + 1) * pack * ch] = block * masks[g]

    place(0, left_own)
    for k in range(1, n_seq):
        left_sends[n_seq - k - 1].wait_recv()
        place(k, left_got.at[k - 1])

    group = math.gcd(half, 4)

    def columns(n):
        for m in range(group):
            slot = n * group + m
            for part in range(n_seq):

                def arrived():
                    pltpu.make_async_remote_copy(
                        src_ref=right_own,
                        dst_ref=slot_at(slot, part),
                        send_sem=rsend_sem.at[0],
                        recv_sem=rrecv_sem.at[slot, part],
                        device_id={"res": my_res, "seq": my_col},
                        device_id_type=MESH,
                    ).wait_recv()

                if part:
                    arrived()
                else:
                    mine = first + slot == my_res
                    pl.when(mine)(keep.wait)
                    pl.when(jnp.logical_not(mine))(arrived)
        got = right_got[pl.ds(n * group, group)].reshape(group * rows, n_seq * LANES)
        outer = dot(got, blocks[...]) * inv_count
        for i in range(res):
            terms[i] = outer[:, i * LANES : (i + 1) * LANES]
        count = group * res
        lhs = jnp.concatenate(
            [
                jnp.concatenate(
                    [
                        terms[i, pl.ds(h, count, stride=high), :].astype(BF16)
                        for h in range(high)
                    ],
                    1,
                )
                for i in range(res)
            ],
            0,
        )
        result = dot(lhs, mixed_ref[...]) + bias_ref[...]
        for i in range(res):
            at = pl.ds(pl.multiple_of(n * count, count), count)
            out_ref[i, at, :] = result[i * count : (i + 1) * count].astype(out_ref.dtype)

    if half == group:
        columns(0)
    else:

        @pl.loop(0, half // group)
        def _(n):
            columns(n)

    for copy in left_sends:
        copy.wait_send()

    def finish_right(n, carry):
        send_right(n + 1).wait_send()
        return carry

    lax.fori_loop(0, n_res - 1, finish_right, 0, unroll=n_res <= 8)

    @pl.when(away != 0)
    def _():
        send_right(0).wait_send()


def on_device(alignment, ln_gain, proj_left, proj_right, out_weight, out_bias):
    n_res, n_seq = lax.axis_size("res"), lax.axis_size("seq")
    seqs, res, width = alignment.shape
    ch = proj_left.shape[1]
    cz = out_weight.shape[1]
    half = n_res // n_seq
    cols = res * half
    pack = LANES // seqs
    rows = res * (ch // pack)
    wide = res * pack * ch
    group = math.gcd(half, 4)
    return pl.pallas_call(
        functools.partial(kernel, n_res, n_seq),
        out_shape=jax.ShapeDtypeStruct((res, cols, cz), BF16),
        in_specs=[pl.BlockSpec(memory_space=pl.ANY)] * 6,
        out_specs=pl.BlockSpec(memory_space=pltpu.VMEM),
        scratch_shapes=[
            pltpu.VMEM((seqs, res, width), BF16),
            pltpu.VMEM((1, width), F32),
            pltpu.VMEM((ch, width), BF16),
            pltpu.VMEM((ch, width), BF16),
            pltpu.VMEM((ch * ch, cz), BF16),
            pltpu.VMEM((1, cz), F32),
            pltpu.VMEM((width // LANES, seqs * res, LANES), F32),
            pltpu.VMEM((ch * ch, cz), F32),
            pltpu.VMEM((ch * ch, cz), BF16),
            pltpu.VMEM((res * seqs, pack * ch), BF16),
            pltpu.VMEM((n_seq - 1, res * seqs, pack * ch), BF16),
            pltpu.VMEM((n_seq * LANES, wide), BF16),
            pltpu.VMEM((rows, LANES), BF16),
            pltpu.VMEM((half, rows, n_seq * LANES), BF16),
            pltpu.VMEM((res, group * rows, LANES), F32),
            pltpu.SemaphoreType.DMA((6,)),
            pltpu.SemaphoreType.DMA((n_seq - 1,)),
            pltpu.SemaphoreType.DMA((n_seq - 1,)),
            pltpu.SemaphoreType.DMA((n_res,)),
            pltpu.SemaphoreType.DMA((half, n_seq)),
            pltpu.SemaphoreType.DMA,
        ],
        compiler_params=pltpu.CompilerParams(collective_id=0, has_side_effects=True),
    )(
        alignment,
        ln_gain.reshape(1, width),
        proj_left.T,
        proj_right.T,
        out_weight,
        out_bias.reshape(1, cz),
    )


def solution(mesh):
    placed = (P(("groups", "seq"), "res", None), P(), P(), P(), P(), P())
    return jax.shard_map(
        on_device,
        mesh=mesh,
        in_specs=placed,
        out_specs=P(("groups", "res"), "seq", None),
        check_vma=False,
    )
```

```python
import functools
import math

import jax
import jax.numpy as jnp
from jax import lax
from jax.experimental import pallas as pl
from jax.experimental.pallas import tpu as pltpu
from jax.sharding import PartitionSpec as P

F32 = jnp.float32
BF16 = jnp.bfloat16
MESH = pl.DeviceIdType.MESH
LANES = 128
SUBLANES = 8


def dot_last(a, b):
    return lax.dot_general(a, b, (((1,), (1,)), ((), ())), preferred_element_type=F32)


def dot(a, b):
    return jnp.dot(a, b, preferred_element_type=F32)


def kernel(
    n_res, n_seq, x_hbm, gain_hbm, wl_hbm, wr_hbm, w_hbm, bias_hbm, out_ref,
    x_ref, gain_ref, wl_ref, wr_ref, w_ref, bias_ref,
    norm_ref, wide_ref, mixed_ref, left_own, left_got, blocks, right_own, right_got, terms,
    load_sem, lsend_sem, lrecv_sem, rsend_sem, rrecv_sem, self_sem,
):
    seqs, res, width = x_ref.shape
    ch = wl_ref.shape[0]
    pack = LANES // seqs
    high = ch // pack
    half = n_res // n_seq
    rows = res * high
    inv_count = 1.0 / (seqs * n_seq)
    my_res, my_seq = lax.axis_index("res"), lax.axis_index("seq")
    my_col = my_res // half
    first = my_seq * half

    loads = [
        pltpu.make_async_copy(src, dst, load_sem.at[n])
        for n, (src, dst) in enumerate(
            (
                (x_hbm, x_ref),
                (gain_hbm, gain_ref),
                (wr_hbm, wr_ref),
                (wl_hbm, wl_ref),
                (w_hbm, w_ref),
                (bias_hbm, bias_ref),
            )
        )
    ]
    for load in loads:
        load.start()

    barrier = pltpu.get_barrier_semaphore()

    def greet(res_at, seq_at):
        pl.semaphore_signal(
            barrier, inc=1, device_id={"res": res_at, "seq": seq_at}, device_id_type=MESH
        )

    for k in range(1, n_seq):
        greet(my_res, lax.rem(my_seq + k, n_seq))

    def greet_block(n, carry):
        res_at = first + n

        for k in range(n_seq):

            @pl.when(res_at != my_res)
            def _():
                greet(res_at, lax.rem(my_seq + k, n_seq))

        return carry

    lax.fori_loop(0, half, greet_block, 0, unroll=half <= 8)

    loads[2].wait()
    at_row = lax.broadcasted_iota(jnp.int32, (ch, ch), 0)
    at_col = lax.broadcasted_iota(jnp.int32, (ch, ch), 1)
    shuffle = (at_col == (at_row % high) * pack + at_row // high).astype(F32).astype(BF16)
    wr_rows = dot(shuffle, wr_ref[...]).astype(BF16)

    loads[0].wait()
    loads[1].wait()
    values = x_ref[...].astype(F32).reshape(seqs * res, width)
    centred = values - jnp.mean(values, axis=-1, keepdims=True)
    variance = jnp.mean(centred * centred, axis=-1, keepdims=True)
    scaled = (centred * lax.rsqrt(variance + 1e-05)) * gain_ref[...]
    for n in range(width // LANES):
        norm_ref[n] = scaled[:, n * LANES : (n + 1) * LANES]
    normed = jnp.concatenate(
        [
            jnp.concatenate(
                [
                    norm_ref[n, pl.ds(i, seqs, stride=res), :].astype(BF16)
                    for n in range(width // LANES)
                ],
                1,
            )
            for i in range(res)
        ],
        0,
    )

    right = dot_last(wr_rows, normed)
    lane_group = lax.broadcasted_iota(jnp.int32, (high, LANES), 1) // seqs
    for j in range(res):
        total = None
        for g in range(pack):
            piece = right[g * high : (g + 1) * high]
            shift = (g - j) * seqs % LANES
            if shift:
                piece = pltpu.roll(piece, shift, 1)
            total = piece if total is None else jnp.where(lane_group == g, piece, total)
        right_own[j * high : (j + 1) * high, :] = total.astype(BF16)

    pl.semaphore_wait(barrier, n_res + n_seq - 2)

    my_slot = lax.rem(my_res, half)
    away = lax.rem(my_seq - my_col + n_seq, n_seq)

    def slot_at(slot, part):
        return right_got.at[slot, :, pl.ds(pl.multiple_of(part * LANES, LANES), LANES)]

    def send_right(step):
        return pltpu.make_async_remote_copy(
            src_ref=right_own,
            dst_ref=slot_at(my_slot, away),
            send_sem=rsend_sem.at[step],
            recv_sem=rrecv_sem.at[my_slot, away],
            device_id={"res": lax.rem(my_res + step, n_res), "seq": my_col},
            device_id_type=MESH,
        )

    def start_right(n, carry):
        send_right(n + 1).start()
        return carry

    lax.fori_loop(0, n_res - 1, start_right, 0, unroll=n_res <= 8)
    keep = pltpu.make_async_copy(right_own, slot_at(my_slot, 0), self_sem)

    @pl.when(away == 0)
    def _():
        keep.start()

    @pl.when(away != 0)
    def _():
        send_right(0).start()

    loads[3].wait()
    wl_wide = jnp.concatenate([wl_ref[...]] * pack, 0)
    left_own[...] = dot_last(normed, wl_wide).astype(BF16)
    left_sends = []
    for k in range(1, n_seq):
        copy = pltpu.make_async_remote_copy(
            src_ref=left_own,
            dst_ref=left_got.at[n_seq - k - 1],
            send_sem=lsend_sem.at[k - 1],
            recv_sem=lrecv_sem.at[n_seq - k - 1],
            device_id={"res": my_res, "seq": lax.rem(my_seq + k, n_seq)},
            device_id_type=MESH,
        )
        copy.start()
        left_sends.append(copy)

    loads[4].wait()
    loads[5].wait()
    wide_ref[...] = w_ref[...].astype(F32)
    for e in range(ch):
        mixed_ref[e * ch : (e + 1) * ch, :] = wide_ref[pl.ds(e, ch, stride=ch), :].astype(BF16)

    masks = [
        (lax.broadcasted_iota(jnp.int32, (seqs, pack * ch), 1) // ch == g).astype(F32).astype(BF16)
        for g in range(pack)
    ]

    def place(part, source):
        for i in range(res):
            block = source[i * seqs : (i + 1) * seqs, :]
            for g in range(pack):
                at = part * LANES + g * seqs
                blocks[at : at + seqs, i * pack * ch : (i + 1) * pack * ch] = block * masks[g]

    place(0, left_own)
    for k in range(1, n_seq):
        left_sends[n_seq - k - 1].wait_recv()
        place(k, left_got.at[k - 1])

    group = math.gcd(half, 4)

    def columns(n):
        for m in range(group):
            slot = n * group + m
            for part in range(n_seq):

                def arrived():
                    pltpu.make_async_remote_copy(
                        src_ref=right_own,
                        dst_ref=slot_at(slot, part),
                        send_sem=rsend_sem.at[0],
                        recv_sem=rrecv_sem.at[slot, part],
                        device_id={"res": my_res, "seq": my_col},
                        device_id_type=MESH,
                    ).wait_recv()

                if part:
                    arrived()
                else:
                    mine = first + slot == my_res
                    pl.when(mine)(keep.wait)
                    pl.when(jnp.logical_not(mine))(arrived)
        got = right_got[pl.ds(n * group, group)].reshape(group * rows, n_seq * LANES)
        outer = dot(got, blocks[...]) * inv_count
        for i in range(res):
            terms[i] = outer[:, i * LANES : (i + 1) * LANES]
        count = group * res
        lhs = jnp.concatenate(
            [
                jnp.concatenate(
                    [
                        terms[i, pl.ds(h, count, stride=high), :].astype(BF16)
                        for h in range(high)
                    ],
                    1,
                )
                for i in range(res)
            ],
            0,
        )
        result = dot(lhs, mixed_ref[...]) + bias_ref[...]
        for i in range(res):
            at = pl.ds(pl.multiple_of(n * count, count), count)
            out_ref[i, at, :] = result[i * count : (i + 1) * count].astype(out_ref.dtype)

    if half == group:
        columns(0)
    else:

        @pl.loop(0, half // group)
        def _(n):
            columns(n)

    for copy in left_sends:
        copy.wait_send()

    def finish_right(n, carry):
        send_right(n + 1).wait_send()
        return carry

    lax.fori_loop(0, n_res - 1, finish_right, 0, unroll=n_res <= 8)

    @pl.when(away != 0)
    def _():
        send_right(0).wait_send()


def on_device(alignment, ln_gain, proj_left, proj_right, out_weight, out_bias):
    n_res, n_seq = lax.axis_size("res"), lax.axis_size("seq")
    seqs, res, width = alignment.shape
    ch = proj_left.shape[1]
    cz = out_weight.shape[1]
    half = n_res // n_seq
    cols = res * half
    pack = LANES // seqs
    rows = res * (ch // pack)
    wide = res * pack * ch
    group = math.gcd(half, 4)
    return pl.pallas_call(
        functools.partial(kernel, n_res, n_seq),
        out_shape=pltpu.VMEM((res, cols, cz), BF16),
        in_specs=[pl.BlockSpec(memory_space=pl.ANY)] * 6,
        out_specs=pl.BlockSpec(memory_space=pltpu.VMEM),
        scratch_shapes=[
            pltpu.VMEM((seqs, res, width), BF16),
            pltpu.VMEM((1, width), F32),
            pltpu.VMEM((ch, width), BF16),
            pltpu.VMEM((ch, width), BF16),
            pltpu.VMEM((ch * ch, cz), BF16),
            pltpu.VMEM((1, cz), F32),
            pltpu.VMEM((width // LANES, seqs * res, LANES), F32),
            pltpu.VMEM((ch * ch, cz), F32),
            pltpu.VMEM((ch * ch, cz), BF16),
            pltpu.VMEM((res * seqs, pack * ch), BF16),
            pltpu.VMEM((n_seq - 1, res * seqs, pack * ch), BF16),
            pltpu.VMEM((n_seq * LANES, wide), BF16),
            pltpu.VMEM((rows, LANES), BF16),
            pltpu.VMEM((half, rows, n_seq * LANES), BF16),
            pltpu.VMEM((res, group * rows, LANES), F32),
            pltpu.SemaphoreType.DMA((6,)),
            pltpu.SemaphoreType.DMA((n_seq - 1,)),
            pltpu.SemaphoreType.DMA((n_seq - 1,)),
            pltpu.SemaphoreType.DMA((n_res,)),
            pltpu.SemaphoreType.DMA((half, n_seq)),
            pltpu.SemaphoreType.DMA,
        ],
        compiler_params=pltpu.CompilerParams(collective_id=0, has_side_effects=True),
    )(
        alignment,
        ln_gain.reshape(1, width),
        proj_left.T,
        proj_right.T,
        out_weight,
        out_bias.reshape(1, cz),
    )


def solution(mesh):
    placed = (P(("groups", "seq"), "res", None), P(), P(), P(), P(), P())
    return jax.shard_map(
        on_device,
        mesh=mesh,
        in_specs=placed,
        out_specs=P(("groups", "res"), "seq", None),
        check_vma=False,
    )
```

```python
import functools
import math

import jax
import jax.numpy as jnp
from jax import lax
from jax.experimental import pallas as pl
from jax.experimental.pallas import tpu as pltpu
from jax.sharding import PartitionSpec as P

F32 = jnp.float32
BF16 = jnp.bfloat16
MESH = pl.DeviceIdType.MESH
LANES = 128
SUBLANES = 8


def dot_last(a, b):
    return lax.dot_general(a, b, (((1,), (1,)), ((), ())), preferred_element_type=F32)


def dot(a, b):
    return jnp.dot(a, b, preferred_element_type=F32)


def kernel(
    n_res, n_seq, x_hbm, gain_hbm, wl_hbm, wr_hbm, w_hbm, bias_hbm, out_ref,
    x_ref, gain_ref, wl_ref, wr_ref, w_ref, bias_ref,
    norm_ref, wide_ref, mixed_ref, left_own, left_got, blocks, right_own, right_got, terms,
    load_sem, lsend_sem, lrecv_sem, rsend_sem, rrecv_sem, self_sem,
):
    seqs, res, width = x_ref.shape
    ch = wl_ref.shape[0]
    pack = LANES // seqs
    high = ch // pack
    half = n_res // n_seq
    rows = res * high
    inv_count = 1.0 / (seqs * n_seq)
    my_res, my_seq = lax.axis_index("res"), lax.axis_index("seq")
    my_col = my_res // half
    first = my_seq * half

    loads = [
        pltpu.make_async_copy(src, dst, load_sem.at[n])
        for n, (src, dst) in enumerate(
            (
                (x_hbm, x_ref),
                (gain_hbm, gain_ref),
                (wr_hbm, wr_ref),
                (wl_hbm, wl_ref),
                (w_hbm, w_ref),
                (bias_hbm, bias_ref),
            )
        )
    ]
    for load in loads[:3]:
        load.start()

    barrier = pltpu.get_barrier_semaphore()

    def greet(res_at, seq_at):
        pl.semaphore_signal(
            barrier, inc=1, device_id={"res": res_at, "seq": seq_at}, device_id_type=MESH
        )

    for k in range(1, n_seq):
        greet(my_res, lax.rem(my_seq + k, n_seq))

    def greet_block(n, carry):
        res_at = first + n

        for k in range(n_seq):

            @pl.when(res_at != my_res)
            def _():
                greet(res_at, lax.rem(my_seq + k, n_seq))

        return carry

    lax.fori_loop(0, half, greet_block, 0, unroll=half <= 8)

    loads[2].wait()
    at_row = lax.broadcasted_iota(jnp.int32, (ch, ch), 0)
    at_col = lax.broadcasted_iota(jnp.int32, (ch, ch), 1)
    shuffle = (at_col == (at_row % high) * pack + at_row // high).astype(F32).astype(BF16)
    wr_rows = dot(shuffle, wr_ref[...]).astype(BF16)

    loads[0].wait()
    loads[1].wait()
    for load in loads[3:]:
        load.start()
    values = x_ref[...].astype(F32).reshape(seqs * res, width)
    centred = values - jnp.mean(values, axis=-1, keepdims=True)
    variance = jnp.mean(centred * centred, axis=-1, keepdims=True)
    scaled = (centred * lax.rsqrt(variance + 1e-05)) * gain_ref[...]
    for n in range(width // LANES):
        norm_ref[n] = scaled[:, n * LANES : (n + 1) * LANES]
    normed = jnp.concatenate(
        [
            jnp.concatenate(
                [
                    norm_ref[n, pl.ds(i, seqs, stride=res), :].astype(BF16)
                    for n in range(width // LANES)
                ],
                1,
            )
            for i in range(res)
        ],
        0,
    )

    right = dot_last(wr_rows, normed)
    lane_group = lax.broadcasted_iota(jnp.int32, (high, LANES), 1) // seqs
    for j in range(res):
        total = None
        for g in range(pack):
            piece = right[g * high : (g + 1) * high]
            shift = (g - j) * seqs % LANES
            if shift:
                piece = pltpu.roll(piece, shift, 1)
            total = piece if total is None else jnp.where(lane_group == g, piece, total)
        right_own[j * high : (j + 1) * high, :] = total.astype(BF16)

    pl.semaphore_wait(barrier, n_res + n_seq - 2)

    my_slot = lax.rem(my_res, half)
    away = lax.rem(my_seq - my_col + n_seq, n_seq)

    def slot_at(slot, part):
        return right_got.at[slot, :, pl.ds(pl.multiple_of(part * LANES, LANES), LANES)]

    def send_right(target):
        return pltpu.make_async_remote_copy(
            src_ref=right_own,
            dst_ref=slot_at(my_slot, away),
            send_sem=rsend_sem.at[target],
            recv_sem=rrecv_sem.at[my_slot, away],
            device_id={"res": target, "seq": my_col},
            device_id_type=MESH,
        )

    def other(target):
        return jnp.logical_or(target != my_res, away != 0)

    def start_right(target, carry):
        pl.when(other(target))(send_right(target).start)
        return carry

    keep = pltpu.make_async_copy(right_own, slot_at(my_slot, 0), self_sem)

    @pl.when(away == 0)
    def _():
        keep.start()

    lax.fori_loop(0, n_res, start_right, 0, unroll=n_res <= 8)

    loads[3].wait()
    wl_wide = jnp.concatenate([wl_ref[...]] * pack, 0)
    left_own[...] = dot_last(normed, wl_wide).astype(BF16)
    left_sends = []
    for k in range(1, n_seq):
        copy = pltpu.make_async_remote_copy(
            src_ref=left_own,
            dst_ref=left_got.at[n_seq - k - 1],
            send_sem=lsend_sem.at[k - 1],
            recv_sem=lrecv_sem.at[n_seq - k - 1],
            device_id={"res": my_res, "seq": lax.rem(my_seq + k, n_seq)},
            device_id_type=MESH,
        )
        copy.start()
        left_sends.append(copy)

    loads[4].wait()
    loads[5].wait()
    wide_ref[...] = w_ref[...].astype(F32)
    for e in range(ch):
        mixed_ref[e * ch : (e + 1) * ch, :] = wide_ref[pl.ds(e, ch, stride=ch), :].astype(BF16)

    masks = [
        (lax.broadcasted_iota(jnp.int32, (seqs, pack * ch), 1) // ch == g).astype(F32).astype(BF16)
        for g in range(pack)
    ]

    def place(part, source):
        for i in range(res):
            block = source[i * seqs : (i + 1) * seqs, :]
            for g in range(pack):
                at = part * LANES + g * seqs
                blocks[at : at + seqs, i * pack * ch : (i + 1) * pack * ch] = block * masks[g]

    place(0, left_own)
    for k in range(1, n_seq):
        left_sends[n_seq - k - 1].wait_recv()
        place(k, left_got.at[k - 1])

    group = math.gcd(half, 4)

    def columns(n):
        for m in range(group):
            slot = n * group + m
            for part in range(n_seq):

                def arrived():
                    pltpu.make_async_remote_copy(
                        src_ref=right_own,
                        dst_ref=slot_at(slot, part),
                        send_sem=rsend_sem.at[0],
                        recv_sem=rrecv_sem.at[slot, part],
                        device_id={"res": my_res, "seq": my_col},
                        device_id_type=MESH,
                    ).wait_recv()

                if part:
                    arrived()
                else:
                    mine = first + slot == my_res
                    pl.when(mine)(keep.wait)
                    pl.when(jnp.logical_not(mine))(arrived)
        got = right_got[pl.ds(n * group, group)].reshape(group * rows, n_seq * LANES)
        outer = dot(got, blocks[...]) * inv_count
        for i in range(res):
            terms[i] = outer[:, i * LANES : (i + 1) * LANES]
        count = group * res
        lhs = jnp.concatenate(
            [
                jnp.concatenate(
                    [
                        terms[i, pl.ds(h, count, stride=high), :].astype(BF16)
                        for h in range(high)
                    ],
                    1,
                )
                for i in range(res)
            ],
            0,
        )
        result = dot(lhs, mixed_ref[...]) + bias_ref[...]
        for i in range(res):
            at = pl.ds(pl.multiple_of(n * count, count), count)
            out_ref[i, at, :] = result[i * count : (i + 1) * count].astype(out_ref.dtype)

    if half == group:
        columns(0)
    else:

        @pl.loop(0, half // group)
        def _(n):
            columns(n)

    for copy in left_sends:
        copy.wait_send()

    def finish_right(target, carry):
        pl.when(other(target))(send_right(target).wait_send)
        return carry

    lax.fori_loop(0, n_res, finish_right, 0, unroll=n_res <= 8)


def on_device(alignment, ln_gain, proj_left, proj_right, out_weight, out_bias):
    n_res, n_seq = lax.axis_size("res"), lax.axis_size("seq")
    seqs, res, width = alignment.shape
    ch = proj_left.shape[1]
    cz = out_weight.shape[1]
    half = n_res // n_seq
    cols = res * half
    pack = LANES // seqs
    rows = res * (ch // pack)
    wide = res * pack * ch
    group = math.gcd(half, 4)
    return pl.pallas_call(
        functools.partial(kernel, n_res, n_seq),
        out_shape=pltpu.VMEM((res, cols, cz), BF16),
        in_specs=[pl.BlockSpec(memory_space=pl.ANY)] * 6,
        out_specs=pl.BlockSpec(memory_space=pltpu.VMEM),
        scratch_shapes=[
            pltpu.VMEM((seqs, res, width), BF16),
            pltpu.VMEM((1, width), F32),
            pltpu.VMEM((ch, width), BF16),
            pltpu.VMEM((ch, width), BF16),
            pltpu.VMEM((ch * ch, cz), BF16),
            pltpu.VMEM((1, cz), F32),
            pltpu.VMEM((width // LANES, seqs * res, LANES), F32),
            pltpu.VMEM((ch * ch, cz), F32),
            pltpu.VMEM((ch * ch, cz), BF16),
            pltpu.VMEM((res * seqs, pack * ch), BF16),
            pltpu.VMEM((n_seq - 1, res * seqs, pack * ch), BF16),
            pltpu.VMEM((n_seq * LANES, wide), BF16),
            pltpu.VMEM((rows, LANES), BF16),
            pltpu.VMEM((half, rows, n_seq * LANES), BF16),
            pltpu.VMEM((res, group * rows, LANES), F32),
            pltpu.SemaphoreType.DMA((6,)),
            pltpu.SemaphoreType.DMA((n_seq - 1,)),
            pltpu.SemaphoreType.DMA((n_seq - 1,)),
            pltpu.SemaphoreType.DMA((n_res,)),
            pltpu.SemaphoreType.DMA((half, n_seq)),
            pltpu.SemaphoreType.DMA,
        ],
        compiler_params=pltpu.CompilerParams(collective_id=0, has_side_effects=True),
    )(
        alignment,
        ln_gain.reshape(1, width),
        proj_left.T,
        proj_right.T,
        out_weight,
        out_bias.reshape(1, cz),
    )


def solution(mesh):
    placed = (P(("groups", "seq"), "res", None), P(), P(), P(), P(), P())
    return jax.shard_map(
        on_device,
        mesh=mesh,
        in_specs=placed,
        out_specs=P(("groups", "res"), "seq", None),
        check_vma=False,
    )
```
